256 devices in a mesh: dp: 32 (over z, y), tp: 8 (over x, core).
Axes of the slice: x: 4, y: 4, z: 8, core: 2. Of those that a mesh axis runs over, the one named last changes fastest.
Arguments:
- tokens: bfloat16 [3072, 2880], P('dp', 'tp'), may hold values from -100 to 100
- attn_gain: float32 [2880], replicated, may hold values from 0.1 to 1.9
- w_query: bfloat16 [2880, 2048], P(None, 'tp'), may hold values from -0.109375 to 0.109375
- w_keyvalue: bfloat16 [2880, 8, 128], P(None, 'tp'), may hold values from -0.109375 to 0.109375
- attn_sinks: float32 [32], P('tp'), may hold values from 2 to 6
- w_out: bfloat16 [2048, 2880], P('tp'), may hold values from -0.125 to 0.125
- window_cache: bfloat16 [3072, 8, 128, 128], P('dp', 'tp'), may hold values from -1000 to 1000
- positions: int32 [3072], P('dp'), may hold values from 0 to 511
- moe_gain: float32 [2880], replicated, may hold values from 0.1 to 1.9
- router: bfloat16 [2880, 32], P('tp'), may hold values from -0.109375 to 0.109375
- gate_up: bfloat16 [32, 2880, 2, 2880], P('dp', None, None, 'tp'), may hold values from -0.109375 to 0.109375
- w_down: bfloat16 [32, 2880, 2880], P('dp', None, 'tp'), may hold values from -0.109375 to 0.109375
- expert_ids: int32 [3072, 4], P('dp'), may hold values from 0 to 31, all different within a row; in each aligned block of 96 rows (0 to 95, 96 to 191, ...) at most 32 rows name the same one
Outputs:
- layer_out: float32 [3072, 2880], P('dp', 'tp')
The draws below stay inside these ranges and needn't reach their ends.
Inputs may be any that keep to these rules, and one draw needn't show every extreme that they name: `expert_ids`: each row names 4 different experts. Within the rows of one index of dp no expert is named by more than 32 rows, a bound that some of these blocks reach.
All inputs are finite; a program needn't handle non-finite values.
Results may differ from the reference program's by a relative error of at most 0.0066.
Values may be sent and summed in bfloat16 or wider, within the bound.
No kernel may reach another device: no remote copies, remote signals or barrier semaphores. Data moves between devices by JAX's collectives and lax.ppermute only.
A program may use at most 128 MiB of HBM per device.

```python
import math
import jax
import jax.numpy as jnp
import numpy as np
from jax import lax

D = 2880
QH = 32
KVH = 8
HD = 64
WINDOW = 128
TOP = 4
FF = 2880
TOK_DEV = 96
EXPERTS = 32
TOKENS = 3072
CAP = 32
N_DP = 32


def draw_tokens(key, part):
    base_key, col_key, row_key = jax.random.split(key, 3)
    places = jnp.arange(D, dtype=jnp.float32) / D
    col_scale = jnp.power(10.0, 0.5 * places + 0.5 * jax.random.uniform(col_key, (D,)))
    base = jnp.clip(jax.random.normal(base_key, (TOKENS, D)), -4.0, 4.0)
    row_scale = jnp.power(10.0, jax.random.uniform(row_key, (TOKENS, 1)))
    return (0.1 * base * row_scale * col_scale[None, :]).astype(jnp.bfloat16)


def draw_window_cache(key, part):
    normal_key = jax.random.fold_in(key, 0)
    entries = jnp.clip(jax.random.normal(normal_key, (TOKENS, KVH, WINDOW, 2 * HD)), -6.0, 6.0)
    return entries.astype(jnp.bfloat16)


def touch_ends(result, key, smallest, high):
    spot = [jax.random.randint(jax.random.fold_in(key, axis), (), 0, length) for axis, length in enumerate(result.shape)]
    main_axis = result.shape.index(max(result.shape))
    next_to = spot[:main_axis] + [(spot[main_axis] + 1) % result.shape[main_axis]] + spot[main_axis + 1:]
    return result.at[tuple(spot)].set(smallest).at[tuple(next_to)].set(high)


def block_levels(key, extent, shards, smallest, high):
    loudness, own = 1.0, jax.random.fold_in(key, 6)
    for dim, parts in shards:
        draws = jnp.exp(jax.random.uniform(jax.random.fold_in(own, dim), (parts,), jnp.float32, smallest / len(shards), high / len(shards)))
        loudness = loudness * jnp.repeat(draws, extent[dim] // parts).reshape([-1 if axis == dim else 1 for axis in range(len(extent))])
    return loudness


def routed_block(own_key, own, number, rows, number_of, top, reach, slope):
    ranking = jax.random.permutation(own_key, number_of)
    crowded, ordinary = load_shares(number_of, rows * top, reach, slope, True), load_shares(number_of, rows * top, reach, slope, False)
    places = jnp.arange(number_of)

    def named(sizes, turn):
        used = int((sizes > 0).sum())
        fixed = max(1, used // 4)
        moved = fixed + (places - fixed + turn * (used - fixed)) % max(1, number_of - fixed)
        return jnp.zeros((number_of,), jnp.int32).at[ranking[jnp.where(places < fixed, places, moved)]].set(jnp.asarray(sizes, jnp.int32))

    sizes = jnp.where(number % 4 == 0, named(crowded, number // 4), named(ordinary, number - number // 4 - 1))
    mixed = jax.random.permutation(jax.random.fold_in(own, 3), number_of)
    donor, sink = mixed[0:number_of // 2 * 2:2], mixed[1:number_of // 2 * 2:2]
    slack = jnp.minimum(sizes[donor] - 1, reach - sizes[sink]) // 2
    slack = jnp.where((donor == ranking[0]) | (sink == ranking[0]) | (sizes[sink] == 0), 0, jnp.maximum(slack, 0))
    moved = jax.random.randint(jax.random.fold_in(own, 4), (number_of // 2,), 0, 1 << 20) % (slack + 1)
    sizes = sizes.at[donor].add(-moved).at[sink].add(moved)
    items = jnp.searchsorted(jnp.cumsum(sizes), jnp.arange(rows * top), side="right").astype(jnp.int32)
    listing = items.reshape(top, rows).T
    listing = listing[jax.random.permutation(jax.random.fold_in(own, 1), rows)]
    turn = jax.random.randint(jax.random.fold_in(own, 2), (rows, 1), 0, top)
    return jnp.take_along_axis(listing, (jnp.arange(top)[None, :] + turn) % top, axis=1)


def load_shares(number_of, total, limit, lean, full):
    weights = [(1 << 20) // math.isqrt(rank ** lean) + 1 for rank in range(1, number_of + 1)]
    largest = limit if full else min(limit, max(-(-total // number_of), total * weights[0] // sum(weights)))
    least = 1 if total - largest >= number_of - 1 else 0
    counts, surplus = [largest] + [least] * (number_of - 1), total - largest - least * (number_of - 1)
    while surplus > 0:
        candidates = [i for i in range(1, number_of) if counts[i] < largest] or [i for i in range(1, number_of) if counts[i] < limit]
        mass, left = sum([weights[i] for i in candidates]), surplus
        for i in candidates:
            more = min(limit - counts[i], max(1, left * weights[i] // mass), surplus)
            counts[i] = counts[i] + more
            surplus = surplus - more
    return np.array(counts)


def gaussian(stream_key, shape, spread, most, cuts=(), kind=jnp.bfloat16):
    drawn = spread * jax.random.normal(stream_key, shape, jnp.float32)
    if cuts:
        drawn = drawn * block_levels(stream_key, shape, cuts, -0.22, 0.18)
    return jnp.clip(drawn, -most, most).astype(kind)


def setup_inputs(seed: int = 0) -> dict:
    splits = jax.random.split(jax.random.key(seed), 14)
    tokens = draw_tokens(jax.random.fold_in(splits[13], 71), 0)
    attn_gain = jnp.clip(1.0 + 0.18 * jax.random.normal(splits[1], (D,), jnp.float32), 0.1, 1.9)
    w_query = gaussian(splits[2], (D, QH * HD), D ** -0.5, 0.109375, ((1, 8),))
    w_keyvalue = gaussian(splits[3], (D, KVH, 2 * HD), D ** -0.5, 0.109375, ((1, 8),))
    attn_sinks = jnp.clip(2.0 + 4.0 * jax.random.uniform(splits[4], (QH,), jnp.float32) ** block_levels(splits[4], (QH,), ((0, 8),), -0.2, 0.2), 2.0, 6.0)
    w_out = gaussian(splits[5], (QH * HD, D), (QH * HD) ** -0.5, 0.125, ((0, 8),))
    window_cache = draw_window_cache(jax.random.fold_in(splits[13], 71), 0)
    positions = touch_ends(jax.random.randint(splits[7], (TOKENS,), 0, 4 * WINDOW), jax.random.fold_in(splits[7], 1), 0, (4 * WINDOW) - 1).astype(jnp.int32)
    moe_gain = jnp.clip(1.0 + 0.18 * jax.random.normal(splits[8], (D,), jnp.float32), 0.1, 1.9)
    router = gaussian(splits[9], (D, EXPERTS), D ** -0.5, 0.109375, ((0, 8),))
    gate_up = gaussian(splits[10], (EXPERTS, D, 2, FF), D ** -0.5, 0.109375, ((0, 32), (3, 8)))
    w_down = gaussian(splits[11], (EXPERTS, FF, D), FF ** -0.5, 0.109375, ((0, 32), (2, 8)))
    expert_ids_keys = jax.random.split(jax.random.fold_in(splits[12], 1), TOKENS // TOK_DEV)
    expert_ids_turns = jax.random.permutation(jax.random.fold_in(splits[12], 3), TOKENS // TOK_DEV)
    expert_ids = jax.vmap(lambda own, number: routed_block(jax.random.fold_in(splits[12], 2), own, number, TOK_DEV, EXPERTS, TOP, CAP, 2))(expert_ids_keys, expert_ids_turns).reshape((TOKENS, TOP))
    return {"tokens": tokens, "attn_gain": attn_gain, "w_query": w_query, "w_keyvalue": w_keyvalue, "attn_sinks": attn_sinks, "w_out": w_out, "window_cache": window_cache, "positions": positions, "moe_gain": moe_gain, "router": router, "gate_up": gate_up, "w_down": w_down, "expert_ids": expert_ids}


norm_eps = 1e-05
rope_base = 150000.0
glu_alpha = 1.702

def rope_tables(positions, head_size):
    half_size = head_size // 2
    exponent = jnp.arange(half_size, dtype=jnp.float32) * (2.0 / head_size)
    inverse = jnp.power(jnp.float32(rope_base), -exponent)
    angles = positions.astype(jnp.float32)[:, None] * inverse[None, :]
    return (jnp.cos(angles), jnp.sin(angles))

def rotate(values, cosine, sine_table):
    half_size = values.shape[-1] // 2
    first_half = values[..., :half_size]
    second_half = values[..., half_size:]
    return jnp.concatenate([first_half * cosine - second_half * sine_table, second_half * cosine + first_half * sine_table], axis=-1)

def reference(tokens, attn_gain, w_query, w_keyvalue, attn_sinks, w_out, window_cache, positions, moe_gain, router, gate_up, w_down, expert_ids):
    seq_count, full_width = tokens.shape
    head_size = w_keyvalue.shape[2] // 2
    kv_heads = w_keyvalue.shape[1]
    q_heads = w_query.shape[1] // head_size
    group_size = q_heads // kv_heads
    window = window_cache.shape[2]
    tok_wide = tokens.astype(jnp.float32)
    attn_mean = lax.optimization_barrier(jnp.mean(tok_wide * tok_wide, axis=1, keepdims=True))
    normed = (tok_wide * lax.rsqrt(attn_mean + norm_eps) * attn_gain[None, :]).astype(jnp.bfloat16)
    queries = jnp.dot(normed, w_query, preferred_element_type=jnp.float32).reshape(seq_count, q_heads, head_size)
    fresh_rows = jnp.dot(normed, w_keyvalue.reshape(full_width, kv_heads * 2 * head_size), preferred_element_type=jnp.float32)
    fresh_rows = fresh_rows.reshape(seq_count, kv_heads, 2 * head_size)
    cosine, sine_table = rope_tables(positions, head_size)
    rot_queries = rotate(queries, cosine[:, None, :], sine_table[:, None, :]).astype(jnp.bfloat16)
    new_key = rotate(fresh_rows[..., :head_size], cosine[:, None, :], sine_table[:, None, :])
    new_entry = jnp.concatenate([new_key, fresh_rows[..., head_size:]], axis=-1).astype(jnp.bfloat16)
    slot_ids = jnp.arange(window, dtype=jnp.int32)
    is_current = slot_ids[None, :] == (positions % window)[:, None]
    cache_now = jnp.where(is_current[:, None, :, None], new_entry[:, :, None, :], window_cache)
    is_valid = (positions[:, None] - slot_ids[None, :]) % window <= positions[:, None]
    score_scale = head_size ** (-0.5)

    def attend_head(inputs):
        head_cache, head_query, head_sinks = inputs
        key_part = head_cache[..., :head_size].astype(jnp.float32)
        value_part = head_cache[..., head_size:].astype(jnp.float32)
        scores = jnp.einsum('sgh,swh->sgw', head_query.astype(jnp.float32), key_part) * score_scale
        scores = jnp.where(is_valid[:, None, :], scores, -jnp.inf)
        sink_col = head_sinks[None, :, None]
        peak_score = jnp.maximum(lax.optimization_barrier(jnp.max(scores, axis=-1, keepdims=True)), sink_col)
        raised = jnp.exp(scores - peak_score)
        denominator = lax.optimization_barrier(jnp.sum(raised, axis=-1, keepdims=True)) + jnp.exp(sink_col - peak_score)
        prob_bf = (raised / denominator).astype(jnp.bfloat16)
        return jnp.einsum('sgw,swh->sgh', prob_bf.astype(jnp.float32), value_part).astype(jnp.bfloat16)
    grouped = rot_queries.reshape(seq_count, kv_heads, group_size, head_size)
    attended = lax.map(attend_head, (jnp.transpose(cache_now, (1, 0, 2, 3)), jnp.transpose(grouped, (1, 0, 2, 3)), attn_sinks.reshape(kv_heads, group_size)))
    attended = jnp.transpose(attended, (1, 0, 2, 3)).reshape(seq_count, q_heads * head_size)
    residual = tok_wide + jnp.dot(attended, w_out, preferred_element_type=jnp.float32)
    moe_mean = lax.optimization_barrier(jnp.mean(residual * residual, axis=1, keepdims=True))
    scaled = residual * lax.rsqrt(moe_mean + norm_eps) * moe_gain[None, :]
    logits = jnp.dot(scaled, router.astype(jnp.float32), precision=lax.Precision.HIGHEST)
    hidden_rows = scaled.astype(jnp.bfloat16)
    experts = router.shape[1]
    expert_iota = jnp.arange(experts, dtype=jnp.int32)
    chosen = expert_ids[:, :, None] == expert_iota[None, None, :]
    picked = lax.optimization_barrier(jnp.sum(jnp.where(chosen, logits[:, None, :], 0.0), axis=-1))
    raised_logits = jnp.exp(picked)
    route_weights = raised_logits / lax.optimization_barrier(jnp.sum(raised_logits, axis=1, keepdims=True))
    per_group = seq_count // N_DP
    group_ids = expert_ids.reshape(N_DP, per_group * TOP)
    onehot = (group_ids[:, :, None] == expert_iota[None, None, :]).astype(jnp.int32)
    earlier = jnp.cumsum(onehot, axis=1) - onehot
    slot_of = lax.optimization_barrier(jnp.sum(earlier * onehot, axis=2))
    column = (jnp.arange(N_DP, dtype=jnp.int32)[:, None] * CAP + slot_of).reshape(-1).astype(jnp.int32)
    expert_flat = group_ids.reshape(-1).astype(jnp.int32)
    repeated = jnp.repeat(hidden_rows, TOP, axis=0)
    buffer_rows = jnp.zeros((experts, N_DP * CAP, full_width), jnp.bfloat16).at[expert_flat, column].set(repeated)
    ff_width = w_down.shape[1]

    def one_expert(inputs):
        block_rows, weights_in, weights_down = inputs
        mixed_in = jnp.dot(block_rows, weights_in.reshape(full_width, 2 * ff_width), preferred_element_type=jnp.float32)
        gate_part = mixed_in[:, :ff_width]
        up_part = mixed_in[:, ff_width:]
        act_rows = (gate_part * jax.nn.sigmoid(glu_alpha * gate_part) * (up_part + 1.0)).astype(jnp.bfloat16)
        return jnp.dot(act_rows, weights_down, preferred_element_type=jnp.float32).astype(jnp.bfloat16)
    outputs = lax.map(one_expert, (buffer_rows, gate_up, w_down))
    gathered = outputs[expert_flat, column].reshape(seq_count, TOP, full_width).astype(jnp.float32)
    combined = lax.optimization_barrier(jnp.sum(route_weights[:, :, None] * gathered, axis=1))
    return residual + combined
```

```python
import jax
import jax.numpy as jnp
from jax import lax
from jax.experimental import pallas as pl
from jax.experimental.pallas import tpu as pltpu
from jax.sharding import PartitionSpec as P

norm_eps = 1e-05
rope_base = 150000.0
glu_alpha = 1.702
f32 = jnp.float32
bf16 = jnp.bfloat16


LANE = 128
SLOTS = 32
NEAR = (0, 1, 7)
FAR = (2, 6, 4, 3, 5)


def vmem():
    return pl.BlockSpec(memory_space=pltpu.VMEM)


def smem():
    return pl.BlockSpec(memory_space=pltpu.SMEM)


def call(body, outs, n_smem, args, scratch=()):
    single = not isinstance(outs, (list, tuple))
    return pl.pallas_call(
        body,
        out_shape=outs,
        in_specs=[smem()] * n_smem + [vmem()] * (len(args) - n_smem),
        out_specs=vmem() if single else [vmem()] * len(outs),
        scratch_shapes=list(scratch),
    )(*args)


def shape(dims, dtype):
    return jax.ShapeDtypeStruct(dims, dtype)


X_OFFSETS = (0, 3, 1, 2)


def hop_x(array, step):
    return lax.ppermute(array, "tp", [(i, (i + 2 * step) % 8) for i in range(8)])


def to_sibling(array):
    return lax.ppermute(array, "tp", [(i, i ^ 1) for i in range(8)])


def hop_y(array, step):
    return lax.ppermute(array, "dp", [(i, i - i % 4 + (i + step) % 4) for i in range(32)])


def hop_z(array, step):
    return lax.ppermute(array, "dp", [(i, (i + 4 * step) % 32) for i in range(32)])


def around_y(array):
    return [array, hop_y(array, 1), hop_y(array, 3), hop_y(array, 2)]


def ring_gather(rows):
    half = rows.shape[0] // 2
    right = hop_x(rows, 1)
    left = hop_x(rows, 3)
    other = to_sibling(rows)
    right2 = hop_x(right[:half], 1)
    left2 = hop_x(left[half:], 3)
    own = [rows, right, left, right2, left2]
    return own + [other] + [to_sibling(piece) for piece in own[1:]]


def piece_index(pos, x, core):
    own_core = core if pos < 4 else 1 - core
    return 2 * ((x + X_OFFSETS[pos % 4]) % 4) + own_core


def prepare_body(place, gate_up, w_down, up_out, down_out):
    x, core = place[0], place[1]
    count = gate_up.shape[2] // 8
    wide = up_out.shape[1] // 8
    half = up_out.shape[0] // 2
    pad_rows = half - count
    zero = jnp.zeros((pad_rows, up_out.shape[1]), bf16)
    up_out[count:half, :] = zero
    up_out[half + count :, :] = zero
    down_out[count:, :] = zero
    pad = jnp.zeros((count, wide - count), bf16)
    for t in range(8):
        offset = (t // 2 - x) % 4
        pos = jnp.where(offset == 3, 1, jnp.where(offset == 0, 0, offset + 1))
        pos = pos + jnp.where(core == t % 2, 0, 4)
        spot = pl.ds(pl.multiple_of(pos * wide, LANE), wide)
        lanes = slice(t * count, (t + 1) * count)
        up_out[0:count, spot] = jnp.concatenate([gate_up[0, :, lanes], pad], axis=1)
        up_out[half : half + count, spot] = jnp.concatenate([gate_up[1, :, lanes], pad], axis=1)
        down_out[0:count, spot] = jnp.concatenate([w_down[:, lanes], pad], axis=1)


def turn_halves(values):
    wide = values.shape[1]
    lane = lax.broadcasted_iota(jnp.int32, values.shape, 1) % 64
    ahead = pltpu.roll(values, wide - 32, 1)
    behind = pltpu.roll(values, 32, 1)
    return jnp.where(lane < 32, ahead, behind)


def project_body(place, own, other, gain, w_query, w_kv, cosine, sine, q_out, entry_out):
    x, core = place[0], place[1]
    count = own.shape[2]
    pieces = [own[p].astype(f32) for p in range(4)] + [other[p].astype(f32) for p in range(4)]
    total = sum(jnp.sum(piece * piece, axis=1, keepdims=True) for piece in pieces)
    scale = lax.rsqrt(total / (8 * count) + norm_eps)
    queries = jnp.zeros((own.shape[1], w_query.shape[1]), f32)
    fresh = jnp.zeros((own.shape[1], w_kv.shape[1]), f32)
    for pos in range(8):
        t = piece_index(pos, x, core)
        normed = (pieces[pos] * scale * gain[pl.ds(t, 1), :]).astype(bf16)
        rows = pl.ds(pl.multiple_of(t * count, 8), count)
        queries += jnp.dot(normed, w_query[rows, :], preferred_element_type=f32)
        fresh += jnp.dot(normed, w_kv[rows, :], preferred_element_type=f32)
    cos2, sin2 = cosine[...], sine[...]
    cos4 = jnp.concatenate([cos2, cos2], axis=1)
    sin4 = jnp.concatenate([sin2, sin2], axis=1)
    q_out[...] = (queries * cos4 + turn_halves(queries) * sin4).astype(bf16)
    turned = fresh * cos2 + turn_halves(fresh) * sin2
    lane = lax.broadcasted_iota(jnp.int32, fresh.shape, 1)
    entry_out[...] = jnp.where(lane < 64, turned, fresh).astype(bf16)


def project_out_body(place, attended, w_out, own_out, other_out):
    x, core = place[0], place[1]
    count = w_out.shape[0] // 8
    pad = jnp.zeros((attended.shape[0], own_out.shape[2] - count), f32)
    for pos in range(8):
        t = piece_index(pos, x, core)
        rows = pl.ds(pl.multiple_of(t * count, 8), count)
        part = lax.dot_general(
            attended[...], w_out[rows, :], (((1,), (1,)), ((), ())), preferred_element_type=f32
        )
        part = jnp.concatenate([part, pad], axis=1)
        if pos < 4:
            own_out[pos] = part
        else:
            other_out[pos - 4] = part.astype(bf16)


def select_body(picks0, picks1, picks2, picks3, rows0, rows1, rows2, rows3, *outs):
    slot = lax.broadcasted_iota(jnp.int32, (SLOTS, rows0.shape[0]), 0).astype(f32)
    for j, (picks, rows) in enumerate(
        zip((picks0, picks1, picks2, picks3), (rows0, rows1, rows2, rows3))
    ):
        hits = [jnp.where(slot == picks[dz : dz + 1, :], 1.0, 0.0) for dz in range(8)]
        placed = jnp.dot(
            jnp.concatenate(hits, axis=0).astype(bf16), rows[...], preferred_element_type=f32
        ).astype(bf16)
        for dz in range(8):
            outs[dz][j * SLOTS : (j + 1) * SLOTS, :] = placed[dz * SLOTS : (dz + 1) * SLOTS]


def gathered_rows(refs, lower, upper):
    half = refs[3].shape[0]
    pieces = []
    for group in (refs[:5], refs[5:]):
        pieces += [group[k][lower:upper, :] for k in range(3)]
        if lower < half:
            pieces.append(group[3][lower:upper, :])
        else:
            pieces.append(group[4][lower - half : upper - half, :])
    return pieces


def up_body(*refs):
    pieces_in, weights, out = refs[:10], refs[10], refs[11]
    rows = out.shape[0]
    wide = out.shape[1]
    count = wide - wide // 16
    block = pieces_in[3].shape[0] // 2
    for low in range(0, rows, block):
        pieces = gathered_rows(pieces_in, low, low + block)
        tails = sum(piece[:, wide - LANE :].astype(f32) for piece in pieces)
        lane = lax.broadcasted_iota(jnp.int32, tails.shape, 1) + (wide - LANE)
        keep = (lane >= count) & (lane < count + 3)
        total = jnp.sum(jnp.where(keep, tails, 0.0), axis=1, keepdims=True)
        scale = lax.rsqrt(total / (8 * count) + norm_eps)
        mixed = lax.dot_general(
            jnp.concatenate(pieces, axis=1),
            weights[...],
            (((1,), (1,)), ((), ())),
            preferred_element_type=f32,
        )
        gate = mixed[:, :wide] * scale
        up = mixed[:, wide:] * scale
        act = gate * jax.nn.sigmoid(glu_alpha * gate) * (up + 1.0)
        out[low : low + block, :] = act.astype(bf16)


def down_body(*refs):
    pieces_in, weights, outs = refs[:10], refs[10], refs[11:]
    block = outs[0].shape[0]
    half = pieces_in[3].shape[0]
    for k, out in enumerate(outs):
        cuts = [k * block, (k + 1) * block]
        if cuts[0] < half < cuts[1]:
            cuts.insert(1, half)
        for low, high in zip(cuts, cuts[1:]):
            rows = jnp.concatenate(gathered_rows(pieces_in, low, high), axis=1)
            made = lax.dot_general(
                rows, weights[...], (((1,), (1,)), ((), ())), preferred_element_type=f32
            )
            out[low - k * block : high - k * block, :] = made.astype(bf16)


def combine_body(picks0, picks1, picks2, picks3, w0, w1, w2, w3, *refs):
    backs, outs = refs[:8], refs[8:]
    slot = lax.broadcasted_iota(jnp.int32, (SLOTS, picks0.shape[1]), 0).astype(f32)
    for j, (picks, weight, out) in enumerate(
        zip((picks0, picks1, picks2, picks3), (w0, w1, w2, w3), outs)
    ):
        spread = [
            jnp.where(slot == picks[dz : dz + 1, :], weight[dz : dz + 1, :], 0.0)
            for dz in range(8)
        ]
        spread = jnp.concatenate(spread, axis=0)
        high = spread.astype(bf16)
        low = (spread - high.astype(f32)).astype(bf16)
        rows = jnp.concatenate([backs[dz][j * SLOTS : (j + 1) * SLOTS, :] for dz in range(8)], 0)
        dims = (((0,), (0,)), ((), ()))
        made = lax.dot_general(high, rows, dims, preferred_element_type=f32)
        made += lax.dot_general(low, rows, dims, preferred_element_type=f32)
        out[...] = made.astype(out.dtype)


def rope_tables(positions, head_size):
    half_size = head_size // 2
    exponent = jnp.arange(half_size, dtype=f32) * (2.0 / head_size)
    inverse = jnp.power(f32(rope_base), -exponent)
    angles = positions.astype(f32)[:, None] * inverse[None, :]
    return (jnp.cos(angles), jnp.sin(angles))


def on_device(
    tokens,
    attn_gain,
    w_query,
    w_keyvalue,
    attn_sinks,
    w_out,
    window_cache,
    positions,
    moe_gain,
    router,
    gate_up,
    w_down,
    expert_ids,
):
    seq_count, count = tokens.shape
    wide = -(-count // LANE) * LANE
    full_width = 8 * count
    head_size = w_keyvalue.shape[2] // 2
    group = w_query.shape[1] // head_size
    window = window_cache.shape[2]
    tp_index = lax.axis_index("tp")
    dp_index = lax.axis_index("dp")
    place = jnp.stack([tp_index // 2, tp_index % 2]).astype(jnp.int32)
    moe_slice = lax.dynamic_slice_in_dim(moe_gain, tp_index * count, count)

    own = jnp.stack([tokens, hop_x(tokens, 1), hop_x(tokens, 3), hop_x(tokens, 2)])
    other = to_sibling(own)

    experts = router.shape[1]
    expert_iota = jnp.arange(experts, dtype=jnp.int32)
    chosen = jnp.any(expert_ids[None, :, :] == expert_iota[:, None, None], axis=2)
    before = (
        jnp.arange(seq_count)[:, None] < jnp.arange(seq_count)[None, :]
    ).astype(bf16)
    rank = jnp.dot(chosen.astype(bf16), before, preferred_element_type=f32)
    slots = jnp.where(chosen, rank, -1.0)
    targets = ((dp_index // 4 + jnp.arange(8)) % 8) * 4 + dp_index % 4

    def toward(array):
        grid = array.reshape(8, 4, seq_count)
        column = lax.dynamic_index_in_dim(grid, dp_index % 4, 1, keepdims=False)
        return lax.dynamic_slice_in_dim(
            jnp.concatenate([column, column]), dp_index // 4, 8
        )

    picks = [toward(a) for a in around_y(slots)]

    up_weights, down_weights = call(
        prepare_body,
        [shape((2 * wide, 8 * wide), bf16), shape((wide, 8 * wide), bf16)],
        1,
        [place, jnp.transpose(gate_up[0], (1, 2, 0)), jnp.transpose(w_down[0])],
    )

    cosine, sine = rope_tables(positions, head_size)
    cos2 = jnp.concatenate([cosine] * 4, axis=1)
    sin2 = jnp.concatenate([-sine, sine] * 2, axis=1)
    rot_queries, new_entry = call(
        project_body,
        [shape((seq_count, group * head_size), bf16), shape((seq_count, 2 * head_size), bf16)],
        1,
        [
            place,
            own,
            other,
            attn_gain.reshape(8, count),
            w_query,
            w_keyvalue.reshape(full_width, 2 * head_size),
            cos2,
            sin2,
        ],
    )

    slot_ids = jnp.arange(window, dtype=jnp.int32)
    is_current = slot_ids[None, :] == (positions % window)[:, None]
    is_valid = (positions[:, None] - slot_ids[None, :]) % window <= positions[:, None]
    cache = window_cache[:, 0]
    grouped = rot_queries.reshape(seq_count, group, head_size)
    scores = jnp.einsum(
        "sgh,swh->sgw", grouped, cache[..., :head_size], preferred_element_type=f32
    )
    fresh_score = jnp.sum(
        grouped.astype(f32) * new_entry[:, None, :head_size].astype(f32), axis=-1, keepdims=True
    )
    scores = jnp.where(is_current[:, None, :], fresh_score, scores) * head_size ** (-0.5)
    scores = jnp.where(is_valid[:, None, :], scores, -jnp.inf)
    sink_col = attn_sinks[None, :, None]
    peak_score = jnp.maximum(jnp.max(scores, axis=-1, keepdims=True), sink_col)
    raised = jnp.exp(scores - peak_score)
    denominator = jnp.sum(raised, axis=-1, keepdims=True) + jnp.exp(sink_col - peak_score)
    prob_bf = (raised / denominator).astype(bf16)
    old_prob = jnp.where(is_current[:, None, :], 0.0, prob_bf).astype(bf16)
    fresh_prob = jnp.sum(
        jnp.where(is_current[:, None, :], prob_bf.astype(f32), 0.0), axis=-1, keepdims=True
    )
    attended = jnp.einsum(
        "sgw,swh->sgh", old_prob, cache[..., head_size:], preferred_element_type=f32
    )
    attended = attended + fresh_prob * new_entry[:, None, head_size:].astype(f32)
    attended = attended.astype(bf16).reshape(seq_count, group * head_size)

    own_part, other_part = call(
        project_out_body,
        [shape((4, seq_count, wide), f32), shape((4, seq_count, wide), bf16)],
        1,
        [place, attended, jnp.transpose(w_out)],
    )
    pair = own_part + to_sibling(other_part).astype(f32)
    sent = pair[1:].astype(bf16)
    arrived = [hop_x(sent[0], 3), hop_x(sent[1], 1), hop_x(sent[2], 2)]
    summed = pair[0] + sum(part.astype(f32) for part in arrived)
    residual = tokens.astype(f32) + summed[:, :count]

    moe_sq = jnp.sum(residual * residual, axis=1, keepdims=True)
    gained = residual * moe_slice[None, :]
    sq_high = moe_sq.astype(bf16)
    sq_rest = moe_sq - sq_high.astype(f32)
    sq_mid = sq_rest.astype(bf16)
    sq_low = (sq_rest - sq_mid.astype(f32)).astype(bf16)
    rows = jnp.concatenate(
        [
            gained.astype(bf16),
            sq_high,
            sq_mid,
            sq_low,
            jnp.zeros((seq_count, wide - count - 3), bf16),
        ],
        axis=1,
    )
    blocks = around_y(rows)
    placed = call(
        select_body, [shape((4 * SLOTS, wide), bf16)] * 8, 0, picks + blocks
    )
    received = [placed[0]] + [None] * 7
    for dz in NEAR[1:] + FAR:
        received[dz] = hop_z(placed[dz], dz)

    partial_logits = jnp.dot(gained, router.astype(f32), precision=lax.Precision.HIGHEST)
    small = jnp.concatenate([partial_logits, moe_sq], axis=1)
    small = small + to_sibling(small)
    small = small + hop_x(small, 1) + hop_x(small, 3) + hop_x(small, 2)
    moe_scale = lax.rsqrt(small[:, experts:] / full_width + norm_eps)
    logits = small[:, :experts] * moe_scale
    hit = expert_ids[:, :, None] == expert_iota[None, None, :]
    picked = jnp.sum(jnp.where(hit, logits[:, None, :], 0.0), axis=-1)
    raised_logits = jnp.exp(picked)
    route_weights = raised_logits / jnp.sum(raised_logits, axis=1, keepdims=True)
    dense = jnp.sum(jnp.where(hit, route_weights[:, :, None], 0.0), axis=1)
    route = [toward(a) for a in around_y(jnp.transpose(dense))]

    acts = {}
    for part in (NEAR, FAR):
        rows_in = jnp.concatenate([received[dz] for dz in part])
        acts[part] = call(
            up_body, shape(rows_in.shape, bf16), 0, ring_gather(rows_in) + [up_weights]
        )
    backs = [None] * 8
    for part in (FAR, NEAR):
        made = call(
            down_body,
            [shape((4 * SLOTS, wide), bf16)] * len(part),
            0,
            ring_gather(acts[part]) + [down_weights],
        )
        for dz, out in zip(part, made):
            backs[dz] = hop_z(out, 8 - dz) if dz else out

    parts = call(
        combine_body,
        [shape((seq_count, wide), f32)] + [shape((seq_count, wide), bf16)] * 3,
        0,
        picks + route + backs,
    )
    moe_out = (
        parts[0]
        + hop_y(parts[1], 3).astype(f32)
        + hop_y(parts[2], 1).astype(f32)
        + hop_y(parts[3], 2).astype(f32)
    )
    return residual + moe_out[:, :count]


def solution(mesh):
    in_specs = (
        P("dp", "tp"),
        P(),
        P(None, "tp"),
        P(None, "tp", None),
        P("tp"),
        P("tp", None),
        P("dp", "tp", None, None),
        P("dp"),
        P(),
        P("tp", None),
        P("dp", None, None, "tp"),
        P("dp", None, "tp"),
        P("dp", None),
    )
    out_specs = P("dp", "tp")
    return jax.shard_map(
        on_device, mesh=mesh, in_specs=in_specs, out_specs=out_specs, check_vma=False
    )
```

```python
import functools

import jax
import jax.numpy as jnp
from jax import lax
from jax.experimental import pallas as pl
from jax.experimental.pallas import tpu as pltpu
from jax.sharding import PartitionSpec as P

norm_eps = 1e-05
rope_base = 150000.0
glu_alpha = 1.702
f32 = jnp.float32
bf16 = jnp.bfloat16


LANE = 128
SLOTS = 32
BLOCK = 512


def vmem():
    return pl.BlockSpec(memory_space=pltpu.VMEM)


def smem():
    return pl.BlockSpec(memory_space=pltpu.SMEM)


def call(body, outs, n_smem, args, flops=0):
    single = not isinstance(outs, (list, tuple))
    made = [outs] if single else outs
    moved = sum(a.size * a.dtype.itemsize for a in [*args[n_smem:], *made])
    return pl.pallas_call(
        body,
        out_shape=outs,
        in_specs=[smem()] * n_smem + [vmem()] * (len(args) - n_smem),
        out_specs=vmem() if single else [vmem()] * len(outs),
        cost_estimate=pl.CostEstimate(flops=flops, bytes_accessed=moved, transcendentals=0),
        compiler_params=pltpu.CompilerParams(vmem_limit_bytes=int(moved * 1.2) + (6 << 20)),
    )(*args)


def shape(dims, dtype):
    return jax.ShapeDtypeStruct(dims, dtype)


X_OFFSETS = (0, 3, 1, 2)
RING_OFFSETS = (0, 2, 3, 1)


def permute(array, axis, target):
    count = lax.axis_size(axis)
    return lax.ppermute(array, axis, [(i, target(i)) for i in range(count)])


def hop_x(array, step, other_core=0):
    return permute(array, "tp", lambda i: (i + 2 * step) % 8 ^ other_core)


def to_sibling(array):
    return permute(array, "tp", lambda i: i ^ 1)


def hop_apart(array):
    return permute(array, "tp", lambda i: (i + (6 if i % 2 else 2)) % 8)


def exchange(array, axis):
    return lax.all_to_all(array, axis, 0, 0, tiled=True)


def ring_gather(rows):
    first = hop_apart(rows)
    twin = to_sibling(rows)
    second = hop_apart(twin)
    third = hop_apart(first)
    return [
        rows, twin, first, to_sibling(first), second, to_sibling(second), third, to_sibling(third)
    ]


def piece_index(pos, x, core):
    own_core = core if pos < 4 else 1 - core
    return 2 * ((x + X_OFFSETS[pos % 4]) % 4) + own_core


def place_of(t, x, core):
    offset = (t // 2 - x + 4) % 4
    same = core == t % 2
    near = jnp.where(core == 0, 3, 1)
    nearer, further = jnp.where(same, 2, 4), jnp.where(same, 5, 3)
    pos = jnp.where(offset == near, nearer, further)
    pos = jnp.where(offset == 0, jnp.where(same, 0, 1), pos)
    return jnp.where(offset == 2, jnp.where(same, 6, 7), pos)


def prepare_body(place, weights, out):
    x, core = place[0], place[1]
    groups, count, _ = weights.shape
    wide = out.shape[1] // 8
    half = out.shape[0] // groups
    pad = jnp.zeros((count, wide - count), bf16)
    for group in range(groups):
        low = group * half
        out[low + count : low + half, :] = jnp.zeros((half - count, out.shape[1]), bf16)
        for t in range(8):
            pos = place_of(t, x, core)
            spot = pl.ds(pl.multiple_of(pos * wide, LANE), wide)
            part = weights[group, :, t * count : (t + 1) * count]
            out[low : low + count, spot] = jnp.concatenate([part, pad], axis=1)


def turn_halves(values):
    wide = values.shape[1]
    lane = lax.broadcasted_iota(jnp.int32, values.shape, 1) % 64
    ahead = pltpu.roll(values, wide - 32, 1)
    behind = pltpu.roll(values, 32, 1)
    return jnp.where(lane < 32, ahead, behind)


def project_body(place, *refs):
    own, ring, twin, other_ring, gain, w_query, w_kv, cosine, sine, q_out, entry_out = refs
    x, core = place[0], place[1]
    seqs, count = own.shape
    refs = [own, *(ring.at[k] for k in range(3)), twin, *(other_ring.at[k] for k in range(3))]
    pieces = [ref[...].astype(f32) for ref in refs]
    total = sum(jnp.sum(piece * piece, axis=1, keepdims=True) for piece in pieces)
    scale = lax.rsqrt(total / (8 * count) + norm_eps)
    queries = jnp.zeros((seqs, w_query.shape[1]), f32)
    fresh = jnp.zeros((seqs, w_kv.shape[1]), f32)
    for pos in range(8):
        t = 2 * ((x + RING_OFFSETS[pos % 4]) % 4) + (core if pos < 4 else 1 - core)
        normed = (pieces[pos] * scale * gain[pl.ds(t, 1), :]).astype(bf16)
        rows = pl.ds(pl.multiple_of(t * count, 8), count)
        queries += jnp.dot(normed, w_query[rows, :], preferred_element_type=f32)
        fresh += jnp.dot(normed, w_kv[rows, :], preferred_element_type=f32)
    cos2, sin2 = cosine[...], sine[...]
    cos4 = jnp.concatenate([cos2, cos2], axis=1)
    sin4 = jnp.concatenate([sin2, sin2], axis=1)
    q_out[...] = (queries * cos4 + turn_halves(queries) * sin4).astype(bf16)
    turned = fresh * cos2 + turn_halves(fresh) * sin2
    lane = lax.broadcasted_iota(jnp.int32, fresh.shape, 1)
    entry_out[...] = jnp.where(lane < 64, turned, fresh).astype(bf16)


def project_out_body(place, attended, w_out, own_out, other_out):
    x, core = place[0], place[1]
    count = w_out.shape[0] // 8
    pad = jnp.zeros((attended.shape[0], own_out.shape[2] - count), f32)
    for pos in range(8):
        t = piece_index(pos, x, core)
        rows = pl.ds(pl.multiple_of(t * count, 8), count)
        part = lax.dot_general(
            attended[...], w_out[rows, :], (((1,), (1,)), ((), ())), preferred_element_type=f32
        )
        part = jnp.concatenate([part, pad], axis=1)
        if pos < 4:
            own_out[pos] = part
        else:
            other_out[pos - 4] = part.astype(bf16)


SQUARES, IDS, LOGITS = 0, 3, 7


def split3(values):
    high = values.astype(bf16)
    rest = values - high.astype(f32)
    mid = rest.astype(bf16)
    return [high, mid, (rest - mid.astype(f32)).astype(bf16)]


def select_body(keys, rows, out):
    spot = lax.broadcasted_iota(jnp.int32, (out.shape[0], rows.shape[0]), 0).astype(f32)
    hits = spot == keys[0:1, :]
    for k in range(1, keys.shape[0]):
        hits = hits | (spot == keys[k : k + 1, :])
    placed = jnp.dot(
        jnp.where(hits, 1.0, 0.0).astype(bf16), rows[...], preferred_element_type=f32
    )
    out[...] = placed.astype(bf16)


def in_blocks(rows, work):
    def step(i, carry):
        work(pl.ds(pl.multiple_of(i * BLOCK, BLOCK), BLOCK))
        return carry

    lax.fori_loop(0, rows // BLOCK, step, 0)


def times(pieces, weights, start):
    wide = pieces[0].shape[1]
    return lax.dot_general(
        jnp.concatenate(pieces, axis=1),
        weights[:, start * wide : (start + len(pieces)) * wide],
        (((1,), (1,)), ((), ())),
        preferred_element_type=f32,
    )


def tail_of(pieces):
    return sum(piece[:, piece.shape[1] - LANE :].astype(f32) for piece in pieces)


def partial_body(start, n_pieces, tailed, *refs):
    pieces_in, weights, refs = refs[:n_pieces], refs[n_pieces], refs[n_pieces + 1 :]
    size = 2 if tailed else 1
    before, outs = refs[: len(refs) - size], refs[len(refs) - size :]

    def work(rows):
        pieces = [piece[rows, :] for piece in pieces_in]
        made = times(pieces, weights, start)
        if tailed:
            tails = tail_of(pieces)
            outs[1][rows, :] = tails + before[1][rows, :] if before else tails
        outs[0][rows, :] = made + before[0][rows, :] if before else made

    in_blocks(pieces_in[0].shape[0], work)


def up_body(count, start, place, *refs):
    pieces_in, weights, before, tails_in, out, route_out = refs[:2], *refs[2:]
    wide = out.shape[1]
    expert = place[2].astype(f32)

    def work(rows):
        pieces = [piece[rows, :] for piece in pieces_in]
        tails = tail_of(pieces) + tails_in[rows, :]
        lane = lax.broadcasted_iota(jnp.int32, tails.shape, 1) + (wide - LANE) - count

        def among(start, size):
            return (lane >= start) & (lane < start + size)

        def total(kept, values):
            return jnp.sum(jnp.where(kept, values, 0.0), axis=1, keepdims=True)

        scale = lax.rsqrt(total(among(SQUARES, 3), tails) / (8 * count) + norm_eps)
        logits = tails + pltpu.roll(tails, LANE - 4, 1) + pltpu.roll(tails, LANE - 8, 1)
        raised = jnp.exp(jnp.where(among(LOGITS, 4), logits * scale, 0.0))
        named = pltpu.roll(tails, LOGITS - IDS, 1) == 8.0 * expert
        route = total(among(LOGITS, 4) & named, raised) / total(among(LOGITS, 4), raised)
        route_out[rows, :] = jnp.broadcast_to(route, (route.shape[0], LANE))
        mixed = times(pieces, weights, start) + before[rows, :]
        gate = mixed[:, :wide] * scale
        up = mixed[:, wide:] * scale
        act = gate * jax.nn.sigmoid(glu_alpha * gate) * (up + 1.0)
        out[rows, :] = act.astype(bf16)

    in_blocks(out.shape[0], work)


def down_body(start, *refs):
    pieces_in, weights, before, route, out = refs[:2], *refs[2:]

    def work(rows):
        made = times([piece[rows, :] for piece in pieces_in], weights, start)
        out[rows, :] = ((made + before[rows, :]) * route[rows, :1]).astype(bf16)

    in_blocks(out.shape[0], work)


def combine_body(keys, back, residual, out):
    spot = lax.broadcasted_iota(jnp.int32, (keys.shape[0], back.shape[0]), 1).astype(f32)
    hits = spot == keys[:, 0:1]
    for k in range(1, keys.shape[1]):
        hits = hits | (spot == keys[:, k : k + 1])
    made = jnp.dot(
        jnp.where(hits, 1.0, 0.0).astype(bf16), back[...], preferred_element_type=f32
    )
    out[...] = residual[...] + made[:, : out.shape[1]]


def rope_tables(positions, head_size):
    half_size = head_size // 2
    exponent = jnp.arange(half_size, dtype=f32) * (2.0 / head_size)
    inverse = jnp.power(f32(rope_base), -exponent)
    angles = positions.astype(f32)[:, None] * inverse[None, :]
    return (jnp.cos(angles), jnp.sin(angles))


def on_device(
    tokens,
    attn_gain,
    w_query,
    w_keyvalue,
    attn_sinks,
    w_out,
    window_cache,
    positions,
    moe_gain,
    router,
    gate_up,
    w_down,
    expert_ids,
):
    seq_count, count = tokens.shape
    wide = -(-count // LANE) * LANE
    full_width = 8 * count
    head_size = w_keyvalue.shape[2] // 2
    group = w_query.shape[1] // head_size
    window = window_cache.shape[2]
    tp_index = lax.axis_index("tp")
    dp_index = lax.axis_index("dp")
    place = jnp.stack([tp_index // 2, tp_index % 2, dp_index])
    place = place.astype(jnp.int32)
    ring = [hop_x(tokens, 2), hop_x(tokens, 1), hop_x(tokens, 3)]
    twin = to_sibling(tokens)
    ring = jnp.stack(ring)
    other_ring = to_sibling(ring)

    up_weights = call(
        prepare_body,
        shape((2 * wide, 8 * wide), bf16),
        1,
        [place, jnp.transpose(gate_up[0], (1, 2, 0))],
        flops=int(5e9),
    )
    down_weights = call(
        prepare_body,
        shape((wide, 8 * wide), bf16),
        1,
        [place, jnp.transpose(w_down, (0, 2, 1))],
        flops=int(2e9),
    )

    cosine, sine = rope_tables(positions, head_size)
    cos2 = jnp.concatenate([cosine] * 4, axis=1)
    sin2 = jnp.concatenate([-sine, sine] * 2, axis=1)
    rot_queries, new_entry = call(
        project_body,
        [shape((seq_count, group * head_size), bf16), shape((seq_count, 2 * head_size), bf16)],
        1,
        [
            place,
            tokens,
            ring,
            twin,
            other_ring,
            attn_gain.reshape(8, count),
            w_query,
            w_keyvalue.reshape(full_width, 2 * head_size),
            cos2,
            sin2,
        ],
    )

    slot_ids = jnp.arange(window, dtype=jnp.int32)
    is_current = slot_ids[None, :] == (positions % window)[:, None]
    is_valid = (positions[:, None] - slot_ids[None, :]) % window <= positions[:, None]
    cache = window_cache[:, 0]
    grouped = rot_queries.reshape(seq_count, group, head_size)
    scores = jnp.einsum(
        "sgh,swh->sgw", grouped, cache[..., :head_size], preferred_element_type=f32
    )
    fresh_score = jnp.sum(
        grouped.astype(f32) * new_entry[:, None, :head_size].astype(f32), axis=-1, keepdims=True
    )
    scores = jnp.where(is_current[:, None, :], fresh_score, scores) * head_size ** (-0.5)
    scores = jnp.where(is_valid[:, None, :], scores, -jnp.inf)
    sink_col = attn_sinks[None, :, None]
    peak_score = jnp.maximum(jnp.max(scores, axis=-1, keepdims=True), sink_col)
    raised = jnp.exp(scores - peak_score)
    denominator = jnp.sum(raised, axis=-1, keepdims=True) + jnp.exp(sink_col - peak_score)
    prob_bf = (raised / denominator).astype(bf16)
    old_prob = jnp.where(is_current[:, None, :], 0.0, prob_bf).astype(bf16)
    fresh_prob = jnp.sum(
        jnp.where(is_current[:, None, :], prob_bf.astype(f32), 0.0), axis=-1, keepdims=True
    )
    attended = jnp.einsum(
        "sgw,swh->sgh", old_prob, cache[..., head_size:], preferred_element_type=f32
    )
    attended = attended + fresh_prob * new_entry[:, None, head_size:].astype(f32)
    attended = attended.astype(bf16).reshape(seq_count, group * head_size)

    own_part, other_part = call(
        project_out_body,
        [shape((4, seq_count, wide), f32), shape((4, seq_count, wide), bf16)],
        1,
        [place, attended, jnp.transpose(w_out)],
    )
    experts = router.shape[1]
    expert_iota = jnp.arange(experts, dtype=jnp.int32)
    ids, gain, _ = lax.optimization_barrier((expert_ids, moe_gain, attended))
    moe_slice = lax.dynamic_slice_in_dim(gain, tp_index * count, count)
    hit = ids[:, :, None] == expert_iota[None, None, :]
    order = jnp.arange(seq_count)
    earlier = (order[:, None] > order[None, :]).astype(bf16)
    rank = jnp.dot(earlier, jnp.any(hit, axis=1).astype(bf16), preferred_element_type=f32)
    slots = jnp.sum(jnp.where(hit, rank[:, None, :], 0.0), axis=-1)

    pair = own_part + to_sibling(other_part).astype(f32)
    sent = pair[1:].astype(bf16)
    arrived = [hop_x(sent[0], 3), hop_x(sent[1], 1), hop_x(sent[2], 2)]
    summed = pair[0] + sum(part.astype(f32) for part in arrived)
    residual = tokens.astype(f32) + summed[:, :count]

    moe_sq = jnp.sum(residual * residual, axis=1, keepdims=True)
    gained = residual * moe_slice[None, :]
    logits = jnp.dot(gained, router.astype(f32), precision=lax.Precision.HIGHEST)
    picked = jnp.sum(jnp.where(hit, logits[:, None, :], 0.0), axis=-1)
    rows = [gained.astype(bf16), *split3(moe_sq), ids.astype(bf16), *split3(picked)]
    rows.append(jnp.zeros((seq_count, wide - count - LOGITS - 12), bf16))
    keys = ids.astype(f32) * SLOTS + slots
    total_slots = experts * SLOTS
    placed = call(
        select_body,
        shape((total_slots, wide), bf16),
        0,
        [jnp.transpose(keys), jnp.concatenate(rows, axis=1)],
    )
    rows_in = exchange(placed.reshape(experts, SLOTS, wide), "dp")
    pieces = ring_gather(rows_in.reshape(total_slots, wide))
    sums = [shape((total_slots, 2 * wide), f32), shape((total_slots, LANE), f32)]
    before = call(
        functools.partial(partial_body, 0, 4, True),
        sums,
        0,
        [*pieces[:4], up_weights],
        flops=int(1e10),
    )
    before = call(
        functools.partial(partial_body, 4, 2, True),
        sums,
        0,
        [*pieces[4:6], up_weights, *before],
        flops=int(5e9),
    )
    acts, routes = call(
        functools.partial(up_body, count, 6),
        [shape((total_slots, wide), bf16), shape((total_slots, LANE), f32)],
        1,
        [place, *pieces[6:], up_weights, *before],
        flops=int(5e9),
    )
    pieces = ring_gather(acts)
    sums = [shape((total_slots, wide), f32)]
    before = call(
        functools.partial(partial_body, 0, 4, False),
        sums,
        0,
        [*pieces[:4], down_weights],
        flops=int(5e9),
    )
    before = call(
        functools.partial(partial_body, 4, 2, False),
        sums,
        0,
        [*pieces[4:6], down_weights, *before],
        flops=int(2e9),
    )
    made = call(
        functools.partial(down_body, 6),
        shape((total_slots, wide), bf16),
        0,
        [*pieces[6:], down_weights, *before, routes],
        flops=int(2e9),
    )
    back = exchange(made.reshape(experts, SLOTS, wide), "dp")
    return call(
        combine_body,
        shape((seq_count, count), f32),
        0,
        [keys, back.reshape(total_slots, wide), residual],
    )


def solution(mesh):
    in_specs = (
        P("dp", "tp"),
        P(),
        P(None, "tp"),
        P(None, "tp", None),
        P("tp"),
        P("tp", None),
        P("dp", "tp", None, None),
        P("dp"),
        P(),
        P("tp", None),
        P("dp", None, None, "tp"),
        P("dp", None, "tp"),
        P("dp", None),
    )
    out_specs = P("dp", "tp")
    return jax.shard_map(
        on_device, mesh=mesh, in_specs=in_specs, out_specs=out_specs, check_vma=False
    )
```
